32 devices in a mesh: dp: 8 (over z, y), comp: 4 (over x, core).
Axes of the slice: x: 2, y: 2, z: 4, core: 2. Of those that a mesh axis runs over, the one named last changes fastest.
Arguments:
- points: float32 [8192, 64], P('dp'), may hold values from -36 to 36
- means: float32 [256, 64], P('comp'), may hold values from -6 to 6
- whiten: float32 [256, 64, 64], P('comp'), may hold values from -0.25 to 2, as said below
- log_weight: float32 [256], P('comp'), may hold values from -4 to 4
Outputs:
- new_means: float32 [256, 64], P('comp')
- new_whiten: float32 [256, 64, 64], P('comp')
- new_log_weight: float32 [256], P('comp')
- point_loglik: float32 [8192], P('dp')
The draws below stay inside these ranges and needn't reach their ends.
Inputs may be any that keep to these rules, and one draw needn't show every extreme that they name: Each whiten[k] is lower triangular with diagonal entries between 0.5 and 2.
All inputs are finite; a program needn't handle non-finite values.
Results may differ from the reference program's by a relative error of at most 0.0003.
Values sent between devices are 32-bit elements; how exact they have to be, the bound alone decides.
A program may use at most 64 MiB of HBM per device.

```python
import math
import jax
import jax.numpy as jnp
from jax import lax

D = 64
K = 256
PTS_DEV = 1024
N_DP = 8


def draw_points(key, part):
    total = PTS_DEV * N_DP
    position = jnp.arange(total, dtype=jnp.float32) / total
    scale = 1.0 + 2.0 * position
    base = jnp.clip(jax.random.normal(key, (total, D), jnp.float32), -6.0, 6.0)
    return base * scale[:, None]


def draw_whiten(key, part):
    first, second = jax.random.split(jax.random.fold_in(key, 11))
    diag = jnp.exp(jax.random.uniform(first, (K, D), jnp.float32, jnp.log(0.5), jnp.log(2.0)))
    lower = jnp.clip(jax.random.normal(second, (K, D, D), jnp.float32) * (0.5 / jnp.sqrt(D * 1.0)), -0.25, 0.25)
    row_index = jnp.arange(D)[:, None]
    col_index = jnp.arange(D)[None, :]
    strict = (col_index < row_index).astype(jnp.float32)
    eye = (col_index == row_index).astype(jnp.float32)
    return lower * strict[None] + diag[:, :, None] * eye[None]


def shard_levels(rng, dims, cuts, least, high):
    level, own = 1.0, jax.random.fold_in(rng, 6)
    for dim, shards_of in cuts:
        steps = jnp.exp(jax.random.uniform(jax.random.fold_in(own, dim), (shards_of,), jnp.float32, least / len(cuts), high / len(cuts)))
        level = level * jnp.repeat(steps, dims[dim] // shards_of).reshape([-1 if axis == dim else 1 for axis in range(len(dims))])
    return level


def gaussian(own_key, extent, scale, most, shards=(), held_as=jnp.bfloat16):
    drawn = scale * jax.random.normal(own_key, extent, jnp.float32)
    if shards:
        drawn = drawn * shard_levels(own_key, extent, shards, -0.22, 0.18)
    return jnp.clip(drawn, -most, most).astype(held_as)


def setup_inputs(seed: int = 0) -> dict:
    splits = jax.random.split(jax.random.key(seed), 5)
    points = draw_points(jax.random.fold_in(splits[4], 71), 0)
    means = gaussian(splits[1], (K, D), 1.0, 6.0, ((0, 4),), jnp.float32)
    whiten = draw_whiten(jax.random.fold_in(splits[4], 71), 0)
    log_weight = gaussian(splits[3], (K,), 1.0, 4.0, ((0, 4),), jnp.float32)
    return {"points": points, "means": means, "whiten": whiten, "log_weight": log_weight}


HIGH = lax.Precision.HIGHEST

def reference(points, means, whiten, log_weight):
    width = points.shape[1]
    offset = jnp.einsum('ked,kd->ke', whiten, means, precision=HIGH)
    logdet = jnp.sum(jnp.log(jnp.diagonal(whiten, axis1=1, axis2=2)), axis=1)
    const = log_weight + logdet - 0.5 * width * math.log(2.0 * math.pi)

    def score(pair):
        factor, shift = pair
        projected = jnp.dot(points, factor.T, precision=HIGH) - shift[None, :]
        return jnp.sum(projected * projected, axis=1)
    distance = lax.map(score, (whiten, offset))
    logp = const[:, None] - 0.5 * distance
    peak = jnp.max(logp, axis=0)
    lse = peak + jnp.log(jnp.sum(jnp.exp(logp - peak[None, :]), axis=0))
    resp = jnp.exp(logp - lse[None, :])
    counts = jnp.sum(resp, axis=1)
    sums = jnp.dot(resp, points, precision=HIGH)

    def scatter_one(weight):
        return jnp.dot((points * weight[:, None]).T, points, precision=HIGH)
    scatter = lax.map(scatter_one, resp)
    grown = counts + 1.0
    new_means = sums / grown[:, None]
    eye = jnp.eye(width, dtype=jnp.float32)
    cov = (scatter - sums[:, :, None] * sums[:, None, :] / grown[:, None, None] + eye[None]) / grown[:, None, None]
    chol = jnp.linalg.cholesky(cov)
    new_whiten = lax.linalg.triangular_solve(chol, jnp.broadcast_to(eye, chol.shape), left_side=True, lower=True)
    new_log_weight = jnp.log(grown / (points.shape[0] + K))
    return (new_means, new_whiten, new_log_weight, lse / width)
```

```python
import functools
import math

import jax
import jax.numpy as jnp
from jax import lax
from jax.experimental import pallas as pl
from jax.experimental.pallas import tpu as pltpu
from jax.sharding import PartitionSpec as P

MESH = pl.DeviceIdType.MESH
F32 = jnp.float32
BF16 = jnp.bfloat16


def split2(v):
    high = v.astype(BF16)
    mid = (v - high.astype(F32)).astype(BF16)
    return high, mid


def split3(v):
    high = v.astype(BF16)
    rest = v - high.astype(F32)
    mid = rest.astype(BF16)
    low = (rest - mid.astype(F32)).astype(BF16)
    return high, mid, low


def lanes(shape):
    return lax.broadcasted_iota(jnp.int32, shape, len(shape) - 1)


def kernel(n_dp, pair, n_comp, total_points, total_k, xt_ref, means_ref, whiten_ref, lw_ref,
           out_ref, tail_ref, lse_ref, lwc_ref, xcat_ref, logp_ref, stat_ref, resp_ref, send_ref, yrecv_ref, recv_ref,
           mat_ref, inv_ref, stat_send, stat_recv, y_send, y_recv, rs_send, rs_recv, ag_send, ag_recv, fw_send, fw_recv):
    local, width = means_ref.shape
    count = xt_ref.shape[1]
    far = n_dp // pair
    own = local // n_dp
    half = width // 2
    quarter = width // 4
    eighth = width // 8
    n_rows = send_ref.shape[2]
    me = lax.axis_index("dp")
    mc = lax.axis_index("comp")
    a, b = me // pair, lax.rem(me, pair)
    other = pair - 1 - b
    partner = a * pair + other

    barrier = pltpu.get_barrier_semaphore()

    def greet(d, carry):
        pl.semaphore_signal(barrier, inc=1, device_id={"dp": lax.rem(me + d, n_dp)}, device_id_type=MESH)
        return carry

    lax.fori_loop(1, n_dp, greet, 0)
    for d in range(1, n_comp):
        pl.semaphore_signal(barrier, inc=1, device_id={"comp": lax.rem(mc + d, n_comp)}, device_id_type=MESH)

    xh, xm, xl = split3(xt_ref[...])
    square = (local, local)
    diagonal = lax.broadcasted_iota(jnp.int32, square, 0) == lax.broadcasted_iota(jnp.int32, square, 1)
    lwc_ref[...] = jnp.sum(jnp.where(diagonal, lw_ref[...], 0.0), axis=1, keepdims=True)
    xcat_ref[...] = jnp.concatenate([xh, xm, xh, xm, xl, xh, xl, xm], axis=0)

    group = 8 if local % 8 == 0 else local

    def score(c, carry):
        rows = pl.ds(pl.multiple_of(c * group, group), group)
        w = whiten_ref[rows]
        m = means_ref[rows, :]
        offset = jnp.sum(w * m[:, None, :], axis=2, keepdims=True).reshape(group * width, 1)
        shape = (group, width, width)
        eye = lax.broadcasted_iota(jnp.int32, shape, 1) == lax.broadcasted_iota(jnp.int32, shape, 2)
        diag = jnp.sum(jnp.where(eye, w, 0.0), axis=1)
        const = lwc_ref[rows, :] + jnp.sum(jnp.log(diag), axis=1, keepdims=True) - 0.5 * width * math.log(2.0 * math.pi)
        wh, wm, wl = split3(w.reshape(group * width, width))
        wcat = jnp.concatenate([wh, wh, wm, wm, wh, wl, wm, wl], axis=1)
        projected = jnp.dot(wcat, xcat_ref[...], preferred_element_type=F32) - offset
        distance = jnp.sum((projected * projected).reshape(group, width, count), axis=1)
        logp_ref[rows, :] = const - 0.5 * distance
        return carry

    lax.fori_loop(0, local // group, score, 0)

    logp = logp_ref[...]
    top = jnp.max(logp, axis=0, keepdims=True)
    stat_ref[0, 0:1, :] = top
    stat_ref[0, 1:2, :] = jnp.sum(jnp.exp(logp - top), axis=0, keepdims=True)

    pl.semaphore_wait(barrier, n_dp - 1 + n_comp - 1)

    def stat_copy(d):
        return pltpu.make_async_remote_copy(
            src_ref=stat_ref.at[0], dst_ref=stat_ref.at[d], send_sem=stat_send.at[d], recv_sem=stat_recv.at[d],
            device_id={"comp": lax.rem(mc + d, n_comp)}, device_id_type=MESH)

    for d in range(1, n_comp):
        stat_copy(d).start()
    for d in range(1, n_comp):
        stat_copy(d).wait()

    peak = stat_ref[0, 0:1, :]
    for d in range(1, n_comp):
        peak = jnp.maximum(peak, stat_ref[d, 0:1, :])
    total = jnp.zeros_like(peak)
    for d in range(n_comp):
        total = total + stat_ref[d, 1:2, :] * jnp.exp(stat_ref[d, 0:1, :] - peak)
    lse = peak + jnp.log(total)
    lse_ref[...] = lse / width
    resp = jnp.exp(logp_ref[...] - lse)
    resp_ref[...] = jnp.concatenate(split3(resp), axis=0)

    contract = (((1,), (1,)), ((), ()))

    def weighted(outer):
        high, mid, low = split3(outer)
        first = lax.dot_general(resp_ref[...], high, contract, preferred_element_type=F32)
        second = lax.dot_general(resp_ref[0:2 * local, :], mid, contract, preferred_element_type=F32)
        third = lax.dot_general(resp_ref[0:local, :], low, contract, preferred_element_type=F32)
        small = (first[2 * local:3 * local] + second[local:2 * local]) + third
        return small + (first[local:2 * local] + second[0:local]) + first[0:local]

    def keep(row, value):
        value = value.reshape(far, pair, own, value.shape[1])
        for side in range(pair):
            send_ref[side, :, pl.ds(row, 1)] = value[:, side][:, None]

    def upper(g, carry):
        t = 2 * g
        parts = [xt_ref[pl.ds(i, 1), :] * xt_ref[...] for i in (t, t + quarter, t + 1, t + 1 + quarter)]
        value = weighted(jnp.concatenate(parts, axis=0))
        keep(t, value[:, 0:2 * width])
        keep(t + 1, value[:, 2 * width:4 * width])
        return carry

    def lower(g, carry):
        t = 2 * g
        right = xt_ref[half:width, :]
        parts = [xt_ref[pl.ds(half + q * eighth + s, 1), :] * right for s in (t, t + 1) for q in range(4)]
        value = weighted(jnp.concatenate(parts, axis=0))
        keep(quarter + t, value[:, 0:2 * width])
        keep(quarter + t + 1, value[:, 2 * width:4 * width])
        return carry

    def y_copy(part, lo, size):
        return pltpu.make_async_remote_copy(
            src_ref=send_ref.at[other, :, pl.ds(lo, size)], dst_ref=yrecv_ref.at[:, pl.ds(lo, size)],
            send_sem=y_send.at[part], recv_sem=y_recv.at[part], device_id={"dp": partner}, device_id_type=MESH)

    def z_copy(part, lo, size, d):
        peer = lax.rem(a + d, far)
        return pltpu.make_async_remote_copy(
            src_ref=send_ref.at[b, peer, pl.ds(lo, size)], dst_ref=recv_ref.at[d, pl.ds(lo, size)],
            send_sem=rs_send.at[part, d], recv_sem=rs_recv.at[part, d],
            device_id={"dp": peer * pair + b}, device_id_type=MESH)

    def z_start(part, lo, size):
        if pair > 1:
            y_copy(part, lo, size).wait()
            send_ref[b, :, lo:lo + size] = send_ref[b, :, lo:lo + size] + yrecv_ref[:, lo:lo + size]

        def step(d, carry):
            z_copy(part, lo, size, d).start()
            return carry
        lax.fori_loop(1, far, step, 0)

    piece = eighth
    step_rows = quarter // 4
    parts = [(2 * piece, piece + 1)] + [(c * step_rows, step_rows) for c in range(4)]
    keep(n_rows - 1, weighted(jnp.concatenate([xt_ref[...], jnp.ones_like(xt_ref[...])], axis=0)))
    for part, (lo, size) in enumerate(parts):
        if part == 0:
            lax.fori_loop(0, piece // 2, lower, 0)
        else:
            lax.fori_loop(lo // 2, (lo + size) // 2, upper, 0)
        if pair > 1:
            y_copy(part, lo, size).start()
        if part > 0:
            z_start(part - 1, *parts[part - 1])
    z_start(len(parts) - 1, *parts[-1])
    for part, (lo, size) in enumerate(parts):
        def step(d, carry, part=part, lo=lo, size=size):
            z_copy(part, lo, size, d).wait()
            return carry
        lax.fori_loop(1, far, step, 0)

    def add(d, acc):
        return acc + recv_ref[d]

    recv_ref[0] = lax.fori_loop(1, far, add, send_ref[b, a])

    lane = lanes((own, 2 * width))
    tail = recv_ref[0, n_rows - 1]
    back = pltpu.roll(tail, width, 1)
    grown_low = back + 1.0
    grown = jnp.where(lane < width, back, tail) + 1.0
    sums = jnp.where(lane < width, tail, 0.0)
    centre = sums / grown
    for i in range(width):
        if i < quarter:
            row = recv_ref[0, i]
        elif i < half:
            row = pltpu.roll(recv_ref[0, i - quarter], width, 1)
        else:
            q, s = divmod(i - half, eighth)
            row = recv_ref[0, quarter + s]
            shift = (half - q * half) % (2 * width)
            if shift:
                row = pltpu.roll(row, shift, 1)
        row = jnp.where(lane < width, row, 0.0) - sums[:, i:i + 1] * centre
        mat_ref[i] = row + jnp.where((lane == i) | (lane == width + i), 1.0, 0.0)

    def spread(row, i):
        return jnp.broadcast_to(row[:, i:i + 1], row.shape)

    for j in range(0, width, 2):
        p, q = mat_ref[j], mat_ref[j + 1]
        cross = spread(p, j + 1)
        inv_p = 1.0 / spread(p, j)
        ratio = cross * inv_p
        clean = q - ratio * p
        inv_q = 1.0 / (spread(q, j + 1) - ratio * cross)
        p_scaled, q_scaled = p * inv_p, clean * inv_q
        inv_ref[j] = pltpu.roll(p, width, 1) * jnp.sqrt(grown * inv_p)
        inv_ref[j + 1] = pltpu.roll(clean, width, 1) * jnp.sqrt(grown * inv_q)
        for i in range(j + 2, width):
            u = spread(p, i)
            v = spread(q, i) - ratio * u
            mat_ref[i] = mat_ref[i] - u * p_scaled - v * q_scaled

    for t in range(quarter):
        first, second = inv_ref[half + t], inv_ref[half + quarter + t]
        packed = jnp.where(lane < width, first, pltpu.roll(second, width, 1))
        out_ref[me, :, pl.ds(t, 1), :] = packed[:, None, :]
    for t in range(eighth):
        packed = inv_ref[t]
        for q in range(1, 4):
            packed = jnp.where((lane >= q * half) & (lane < (q + 1) * half),
                               pltpu.roll(inv_ref[q * eighth + t], q * half, 1), packed)
        out_ref[me, :, pl.ds(quarter + t, 1), :] = packed[:, None, :]
    tail_ref[me] = jnp.where(lane < width, centre, jnp.log(grown / (total_points + total_k)))

    def ag_copies(d):
        to = lax.rem(a + d, far) * pair + b
        return [pltpu.make_async_remote_copy(
            src_ref=ref.at[me], dst_ref=ref.at[me], send_sem=ag_send.at[k, d], recv_sem=ag_recv.at[k, d],
            device_id={"dp": to}, device_id_type=MESH) for k, ref in enumerate((out_ref, tail_ref))]

    def fw_copies(d):
        block = lax.rem(a - d + far, far) * pair + b
        return [pltpu.make_async_remote_copy(
            src_ref=ref.at[block], dst_ref=ref.at[block], send_sem=fw_send.at[k, d], recv_sem=fw_recv.at[k, d],
            device_id={"dp": partner}, device_id_type=MESH) for k, ref in enumerate((out_ref, tail_ref))]

    def ag_start(d, carry):
        for copy in ag_copies(d):
            copy.start()
        return carry

    def forward(d, carry):
        for copy in ag_copies(d):
            copy.wait()
        if pair > 1:
            for copy in fw_copies(d):
                copy.start()
        return carry

    def fw_wait(d, carry):
        for copy in fw_copies(d):
            copy.wait()
        return carry

    lax.fori_loop(1, far, ag_start, 0)
    if pair > 1:
        for copy in fw_copies(0):
            copy.start()
    lax.fori_loop(1, far, forward, 0)
    if pair > 1:
        lax.fori_loop(0, far, fw_wait, 0)


def finish(packed_ref, tail_ref, lse_in_ref, means_ref, factor_ref, lw_ref, lse_ref):
    local, width = means_ref.shape
    half, quarter, eighth = width // 2, width // 4, width // 8
    lse_ref[...] = lse_in_ref[...]
    tail = tail_ref[...]
    means_ref[...] = tail[:, :width]
    square = (local, local)
    diagonal = lax.broadcasted_iota(jnp.int32, square, 0) == lax.broadcasted_iota(jnp.int32, square, 1)
    lw_ref[...] = jnp.sum(jnp.where(diagonal, tail[:, width:width + 1], 0.0), axis=0, keepdims=True)

    def step(k, carry):
        bottom = packed_ref[k, 0:quarter, :]
        factor_ref[k, half:half + quarter, :] = bottom[:, :width]
        factor_ref[k, half + quarter:width, :] = pltpu.roll(bottom, width, 1)[:, :width]
        top = packed_ref[k, quarter:quarter + eighth, :]
        lane = lanes(top.shape)
        for q in range(4):
            row = pltpu.roll(top, (4 - q) * half, 1) if q else top
            factor_ref[k, q * eighth:(q + 1) * eighth, :] = jnp.where(lane < half, row, 0.0)[:, :width]
        return carry

    lax.fori_loop(0, local, step, 0, unroll=8)


def body(n_dp, n_comp, points, means, whiten, log_weight):
    count, width = points.shape
    local = means.shape[0]
    own = local // n_dp
    half, quarter, eighth = width // 2, width // 4, width // 8
    n_rows = quarter + eighth + 1
    pair = 2 if n_dp % 2 == 0 else 1
    far = n_dp // pair
    vmem = pl.BlockSpec(memory_space=pltpu.VMEM)
    shape = jax.ShapeDtypeStruct
    packed, tail, lse = pl.pallas_call(
        functools.partial(kernel, n_dp, pair, n_comp, count * n_dp, local * n_comp),
        out_shape=(shape((n_dp, own, n_rows - 1, 2 * width), F32), shape((n_dp, own, 2 * width), F32), shape((1, count), F32)),
        in_specs=[vmem] * 4,
        out_specs=(vmem,) * 3,
        scratch_shapes=[
            pltpu.VMEM((local, 1), F32),
            pltpu.VMEM((8 * width, count), BF16),
            pltpu.VMEM((local, count), F32),
            pltpu.VMEM((n_comp, 2, count), F32),
            pltpu.VMEM((3 * local, count), BF16),
            pltpu.VMEM((pair, far, n_rows, own, 2 * width), F32),
            pltpu.VMEM((far, n_rows, own, 2 * width), F32),
            pltpu.VMEM((far, n_rows, own, 2 * width), F32),
            pltpu.VMEM((width, own, 2 * width), F32),
            pltpu.VMEM((width, own, 2 * width), F32),
            pltpu.SemaphoreType.DMA((n_comp,)),
            pltpu.SemaphoreType.DMA((n_comp,)),
            pltpu.SemaphoreType.DMA((5,)),
            pltpu.SemaphoreType.DMA((5,)),
            pltpu.SemaphoreType.DMA((5, far)),
            pltpu.SemaphoreType.DMA((5, far)),
            pltpu.SemaphoreType.DMA((2, far)),
            pltpu.SemaphoreType.DMA((2, far)),
            pltpu.SemaphoreType.DMA((2, far)),
            pltpu.SemaphoreType.DMA((2, far)),
        ],
        compiler_params=pltpu.CompilerParams(collective_id=0, has_side_effects=True),
        name="em_step",
    )(points.T, means, whiten, log_weight.reshape(1, local))
    centre, factor, weight, lse = pl.pallas_call(
        finish,
        out_shape=(shape((local, width), F32), shape((local, width, width), F32), shape((1, local), F32), shape((1, count), F32)),
        in_specs=[vmem] * 3,
        out_specs=(vmem,) * 4,
        name="finish",
    )(packed.reshape(local, n_rows - 1, 2 * width), tail.reshape(local, 2 * width), lse)
    return centre, factor, weight.reshape(local), lse.reshape(count)


def solution(mesh):
    n_dp, n_comp = mesh.shape["dp"], mesh.shape["comp"]
    in_specs = (P("dp", None), P("comp", None), P("comp", None, None), P("comp"))
    out_specs = (P("comp", None), P("comp", None, None), P("comp"), P("dp"))
    return jax.shard_map(functools.partial(body, n_dp, n_comp), mesh=mesh, in_specs=in_specs, out_specs=out_specs, check_vma=False)
```

```python
import functools
import math

import jax
import jax.numpy as jnp
from jax import lax
from jax.experimental import pallas as pl
from jax.experimental.pallas import tpu as pltpu
from jax.sharding import PartitionSpec as P

MESH = pl.DeviceIdType.MESH
F32 = jnp.float32
BF16 = jnp.bfloat16


def split2(v):
    high = v.astype(BF16)
    mid = (v - high.astype(F32)).astype(BF16)
    return high, mid


def split3(v):
    high = v.astype(BF16)
    rest = v - high.astype(F32)
    mid = rest.astype(BF16)
    low = (rest - mid.astype(F32)).astype(BF16)
    return high, mid, low


def lanes(shape):
    return lax.broadcasted_iota(jnp.int32, shape, len(shape) - 1)


def kernel(n_dp, pair, n_comp, total_points, total_k, xt_ref, means_ref, whiten_ref, lw_ref,
           out_ref, tail_ref, lse_ref, lwc_ref, xcat_ref, logp_ref, stat_ref, resp_ref, send_ref, yrecv_ref, recv_ref,
           mat_ref, inv_ref, stat_send, stat_recv, y_send, y_recv, rs_send, rs_recv, ag_send, ag_recv, fw_send, fw_recv):
    local, width = means_ref.shape
    count = xt_ref.shape[1]
    far = n_dp // pair
    own = local // n_dp
    half = width // 2
    quarter = width // 4
    eighth = width // 8
    n_rows = send_ref.shape[2]
    me = lax.axis_index("dp")
    mc = lax.axis_index("comp")
    a, b = me // pair, lax.rem(me, pair)
    other = pair - 1 - b
    partner = a * pair + other

    barrier = pltpu.get_barrier_semaphore()

    def greet(d, carry):
        pl.semaphore_signal(barrier, inc=1, device_id={"dp": lax.rem(me + d, n_dp)}, device_id_type=MESH)
        return carry

    lax.fori_loop(1, n_dp, greet, 0)
    for d in range(1, n_comp):
        pl.semaphore_signal(barrier, inc=1, device_id={"comp": lax.rem(mc + d, n_comp)}, device_id_type=MESH)

    xh, xm, xl = split3(xt_ref[...])
    square = (local, local)
    diagonal = lax.broadcasted_iota(jnp.int32, square, 0) == lax.broadcasted_iota(jnp.int32, square, 1)
    lwc_ref[...] = jnp.sum(jnp.where(diagonal, lw_ref[...], 0.0), axis=1, keepdims=True)
    xcat_ref[...] = jnp.concatenate([xh, xm, xh, xm, xl, xh, xl, xm], axis=0)

    group = 8 if local % 8 == 0 else local

    def score(c, carry):
        rows = pl.ds(pl.multiple_of(c * group, group), group)
        w = whiten_ref[rows]
        m = means_ref[rows, :]
        offset = jnp.sum(w * m[:, None, :], axis=2, keepdims=True).reshape(group * width, 1)
        shape = (group, width, width)
        eye = lax.broadcasted_iota(jnp.int32, shape, 1) == lax.broadcasted_iota(jnp.int32, shape, 2)
        diag = jnp.sum(jnp.where(eye, w, 0.0), axis=1)
        const = lwc_ref[rows, :] + jnp.sum(jnp.log(diag), axis=1, keepdims=True) - 0.5 * width * math.log(2.0 * math.pi)
        wh, wm, wl = split3(w.reshape(group * width, width))
        wcat = jnp.concatenate([wh, wh, wm, wm, wh, wl, wm, wl], axis=1)
        projected = jnp.dot(wcat, xcat_ref[...], preferred_element_type=F32) - offset
        distance = jnp.sum((projected * projected).reshape(group, width, count), axis=1)
        logp_ref[rows, :] = const - 0.5 * distance
        return carry

    lax.fori_loop(0, local // group, score, 0)

    logp = logp_ref[...]
    top = jnp.max(logp, axis=0, keepdims=True)
    stat_ref[0, 0:1, :] = top
    stat_ref[0, 1:2, :] = jnp.sum(jnp.exp(logp - top), axis=0, keepdims=True)

    pl.semaphore_wait(barrier, n_dp - 1 + n_comp - 1)

    def stat_copy(d):
        return pltpu.make_async_remote_copy(
            src_ref=stat_ref.at[0], dst_ref=stat_ref.at[d], send_sem=stat_send.at[d], recv_sem=stat_recv.at[d],
            device_id={"comp": lax.rem(mc + d, n_comp)}, device_id_type=MESH)

    for d in range(1, n_comp):
        stat_copy(d).start()
    for d in range(1, n_comp):
        stat_copy(d).wait()

    peak = stat_ref[0, 0:1, :]
    for d in range(1, n_comp):
        peak = jnp.maximum(peak, stat_ref[d, 0:1, :])
    total = jnp.zeros_like(peak)
    for d in range(n_comp):
        total = total + stat_ref[d, 1:2, :] * jnp.exp(stat_ref[d, 0:1, :] - peak)
    lse = peak + jnp.log(total)
    lse_ref[...] = lse / width
    resp = jnp.exp(logp_ref[...] - lse)
    resp_ref[...] = jnp.concatenate(split3(resp), axis=0)

    contract = (((1,), (1,)), ((), ()))

    def weighted(outer):
        high, mid, low = split3(outer)
        first = lax.dot_general(resp_ref[...], high, contract, preferred_element_type=F32)
        second = lax.dot_general(resp_ref[0:2 * local, :], mid, contract, preferred_element_type=F32)
        third = lax.dot_general(resp_ref[0:local, :], low, contract, preferred_element_type=F32)
        small = (first[2 * local:3 * local] + second[local:2 * local]) + third
        return small + (first[local:2 * local] + second[0:local]) + first[0:local]

    def keep(row, value):
        value = value.reshape(far, pair, own, value.shape[1])
        for side in range(pair):
            send_ref[side, :, pl.ds(row, 1)] = value[:, side][:, None]

    def upper(g, carry):
        t = 2 * g
        parts = [xt_ref[pl.ds(i, 1), :] * xt_ref[...] for i in (t, t + quarter, t + 1, t + 1 + quarter)]
        value = weighted(jnp.concatenate(parts, axis=0))
        keep(t, value[:, 0:2 * width])
        keep(t + 1, value[:, 2 * width:4 * width])
        return carry

    def lower(g, carry):
        t = 2 * g
        right = xt_ref[half:width, :]
        parts = [xt_ref[pl.ds(half + q * eighth + s, 1), :] * right for s in (t, t + 1) for q in range(4)]
        value = weighted(jnp.concatenate(parts, axis=0))
        keep(quarter + t, value[:, 0:2 * width])
        keep(quarter + t + 1, value[:, 2 * width:4 * width])
        return carry

    def y_copy(part, lo, size):
        return pltpu.make_async_remote_copy(
            src_ref=send_ref.at[other, :, pl.ds(lo, size)], dst_ref=yrecv_ref.at[:, pl.ds(lo, size)],
            send_sem=y_send.at[part], recv_sem=y_recv.at[part], device_id={"dp": partner}, device_id_type=MESH)

    def z_copy(part, lo, size, d):
        peer = lax.rem(a + d, far)
        return pltpu.make_async_remote_copy(
            src_ref=send_ref.at[b, peer, pl.ds(lo, size)], dst_ref=recv_ref.at[d, pl.ds(lo, size)],
            send_sem=rs_send.at[part, d], recv_sem=rs_recv.at[part, d],
            device_id={"dp": peer * pair + b}, device_id_type=MESH)

    def z_start(part, lo, size):
        if pair > 1:
            y_copy(part, lo, size).wait()
            send_ref[b, :, lo:lo + size] = send_ref[b, :, lo:lo + size] + yrecv_ref[:, lo:lo + size]

        def step(d, carry):
            z_copy(part, lo, size, d).start()
            return carry
        lax.fori_loop(1, far, step, 0)

    piece = eighth
    step_rows = quarter // 4
    parts = [(2 * piece, piece + 1)] + [(c * step_rows, step_rows) for c in range(4)]
    keep(n_rows - 1, weighted(jnp.concatenate([xt_ref[...], jnp.ones_like(xt_ref[...])], axis=0)))
    for part, (lo, size) in enumerate(parts):
        if part == 0:
            lax.fori_loop(0, piece // 2, lower, 0)
        else:
            lax.fori_loop(lo // 2, (lo + size) // 2, upper, 0)
        if pair > 1:
            y_copy(part, lo, size).start()
        if part > 0:
            z_start(part - 1, *parts[part - 1])
    z_start(len(parts) - 1, *parts[-1])
    for part, (lo, size) in enumerate(parts):
        def step(d, carry, part=part, lo=lo, size=size):
            z_copy(part, lo, size, d).wait()
            return carry
        lax.fori_loop(1, far, step, 0)

    def add(d, acc):
        return acc + recv_ref[d]

    recv_ref[0] = lax.fori_loop(1, far, add, send_ref[b, a])

    lane = lanes((own, 2 * width))
    tail = recv_ref[0, n_rows - 1]
    back = pltpu.roll(tail, width, 1)
    grown_low = back + 1.0
    grown = jnp.where(lane < width, back, tail) + 1.0
    sums = jnp.where(lane < width, tail, 0.0)
    centre = sums / grown
    for i in range(width):
        if i < quarter:
            row = recv_ref[0, i]
        elif i < half:
            row = pltpu.roll(recv_ref[0, i - quarter], width, 1)
        else:
            q, s = divmod(i - half, eighth)
            row = recv_ref[0, quarter + s]
            shift = (half - q * half) % (2 * width)
            if shift:
                row = pltpu.roll(row, shift, 1)
        row = jnp.where(lane < width, row, 0.0) - sums[:, i:i + 1] * centre
        mat_ref[i] = row + jnp.where((lane == i) | (lane == width + i), 1.0, 0.0)

    def spread(row, i):
        return jnp.broadcast_to(row[:, i:i + 1], row.shape)

    def piece_of(k, block):
        return tail_ref.at[block] if k == 3 else out_ref.at[block, :, pl.ds(k * eighth, eighth)]

    def ag_copy(k, d):
        to = lax.rem(a + d, far) * pair + b
        return pltpu.make_async_remote_copy(
            src_ref=piece_of(k, me), dst_ref=piece_of(k, me), send_sem=ag_send.at[k, d], recv_sem=ag_recv.at[k, d],
            device_id={"dp": to}, device_id_type=MESH)

    def fw_copy(k, d):
        block = lax.rem(a - d + far, far) * pair + b
        return pltpu.make_async_remote_copy(
            src_ref=piece_of(k, block), dst_ref=piece_of(k, block), send_sem=fw_send.at[k, d], recv_sem=fw_recv.at[k, d],
            device_id={"dp": partner}, device_id_type=MESH)

    def ag_begin(k):
        def step(d, carry):
            ag_copy(k, d).start()
            return carry
        lax.fori_loop(1, far, step, 0)
        if pair > 1:
            fw_copy(k, 0).start()

    def ag_forward(k):
        def step(d, carry):
            ag_copy(k, d).wait()
            if pair > 1:
                fw_copy(k, d).start()
            return carry
        lax.fori_loop(1, far, step, 0)

    def ag_end(k):
        def step(d, carry):
            fw_copy(k, d).wait()
            return carry
        if pair > 1:
            lax.fori_loop(0, far, step, 0)

    def pack_two(k, base):
        for t in range(eighth):
            packed = jnp.where(lane < width, inv_ref[base + t], pltpu.roll(inv_ref[base + eighth + t], width, 1))
            out_ref[me, :, pl.ds(k * eighth + t, 1), :] = packed[:, None, :]
        ag_begin(k)

    def pack_four():
        for t in range(eighth):
            packed = inv_ref[t]
            for q in range(1, 4):
                packed = jnp.where((lane >= q * half) & (lane < (q + 1) * half),
                                   pltpu.roll(inv_ref[q * eighth + t], q * half, 1), packed)
            out_ref[me, :, pl.ds(t, 1), :] = packed[:, None, :]
        ag_begin(0)

    tail_ref[me] = jnp.where(lane < width, centre, jnp.log(grown / (total_points + total_k)))
    ag_begin(3)

    for j in range(0, width, 2):
        p, q = mat_ref[j], mat_ref[j + 1]
        cross = spread(p, j + 1)
        inv_p = 1.0 / spread(p, j)
        ratio = cross * inv_p
        clean = q - ratio * p
        inv_q = 1.0 / (spread(q, j + 1) - ratio * cross)
        p_scaled, q_scaled = p * inv_p, clean * inv_q
        inv_ref[j] = pltpu.roll(p, width, 1) * jnp.sqrt(grown * inv_p)
        inv_ref[j + 1] = pltpu.roll(clean, width, 1) * jnp.sqrt(grown * inv_q)
        for i in range(j + 2, width):
            u = spread(p, i)
            v = spread(q, i) - ratio * u
            mat_ref[i] = mat_ref[i] - u * p_scaled - v * q_scaled
        if j + 2 == half:
            pack_four()
        if j + 2 == half + quarter:
            pack_two(1, half)
            ag_forward(3)
            ag_forward(0)
    pack_two(2, half + quarter)
    ag_forward(1)
    ag_forward(2)
    for k in range(4):
        ag_end(k)


def finish(packed_ref, tail_ref, lse_in_ref, means_ref, factor_ref, lw_ref, lse_ref):
    local, width = means_ref.shape
    half, quarter, eighth = width // 2, width // 4, width // 8
    lse_ref[...] = lse_in_ref[...]
    tail = tail_ref[...]
    means_ref[...] = tail[:, :width]
    square = (local, local)
    diagonal = lax.broadcasted_iota(jnp.int32, square, 0) == lax.broadcasted_iota(jnp.int32, square, 1)
    lw_ref[...] = jnp.sum(jnp.where(diagonal, tail[:, width:width + 1], 0.0), axis=0, keepdims=True)

    def step(k, carry):
        for piece in range(2):
            base = half + piece * quarter
            rows = packed_ref[k, (1 + piece) * eighth:(2 + piece) * eighth, :]
            factor_ref[k, base:base + eighth, :] = rows[:, :width]
            factor_ref[k, base + eighth:base + quarter, :] = pltpu.roll(rows, width, 1)[:, :width]
        top = packed_ref[k, 0:eighth, :]
        lane = lanes(top.shape)
        for q in range(4):
            row = pltpu.roll(top, (4 - q) * half, 1) if q else top
            factor_ref[k, q * eighth:(q + 1) * eighth, :] = jnp.where(lane < half, row, 0.0)[:, :width]
        return carry

    lax.fori_loop(0, local, step, 0, unroll=8)


def body(n_dp, n_comp, points, means, whiten, log_weight):
    count, width = points.shape
    local = means.shape[0]
    own = local // n_dp
    half, quarter, eighth = width // 2, width // 4, width // 8
    n_rows = quarter + eighth + 1
    pair = 2 if n_dp % 2 == 0 else 1
    far = n_dp // pair
    vmem = pl.BlockSpec(memory_space=pltpu.VMEM)
    shape = jax.ShapeDtypeStruct
    packed, tail, lse = pl.pallas_call(
        functools.partial(kernel, n_dp, pair, n_comp, count * n_dp, local * n_comp),
        out_shape=(shape((n_dp, own, n_rows - 1, 2 * width), F32), shape((n_dp, own, 2 * width), F32), shape((1, count), F32)),
        in_specs=[vmem] * 4,
        out_specs=(vmem,) * 3,
        scratch_shapes=[
            pltpu.VMEM((local, 1), F32),
            pltpu.VMEM((8 * width, count), BF16),
            pltpu.VMEM((local, count), F32),
            pltpu.VMEM((n_comp, 2, count), F32),
            pltpu.VMEM((3 * local, count), BF16),
            pltpu.VMEM((pair, far, n_rows, own, 2 * width), F32),
            pltpu.VMEM((far, n_rows, own, 2 * width), F32),
            pltpu.VMEM((far, n_rows, own, 2 * width), F32),
            pltpu.VMEM((width, own, 2 * width), F32),
            pltpu.VMEM((width, own, 2 * width), F32),
            pltpu.SemaphoreType.DMA((n_comp,)),
            pltpu.SemaphoreType.DMA((n_comp,)),
            pltpu.SemaphoreType.DMA((5,)),
            pltpu.SemaphoreType.DMA((5,)),
            pltpu.SemaphoreType.DMA((5, far)),
            pltpu.SemaphoreType.DMA((5, far)),
            pltpu.SemaphoreType.DMA((4, far)),
            pltpu.SemaphoreType.DMA((4, far)),
            pltpu.SemaphoreType.DMA((4, far)),
            pltpu.SemaphoreType.DMA((4, far)),
        ],
        compiler_params=pltpu.CompilerParams(collective_id=0, has_side_effects=True),
        name="em_step",
    )(points.T, means, whiten, log_weight.reshape(1, local))
    centre, factor, weight, lse = pl.pallas_call(
        finish,
        out_shape=(shape((local, width), F32), shape((local, width, width), F32), shape((1, local), F32), shape((1, count), F32)),
        in_specs=[vmem] * 3,
        out_specs=(vmem,) * 4,
        name="finish",
    )(packed.reshape(local, n_rows - 1, 2 * width), tail.reshape(local, 2 * width), lse)
    return centre, factor, weight.reshape(local), lse.reshape(count)


def solution(mesh):
    n_dp, n_comp = mesh.shape["dp"], mesh.shape["comp"]
    in_specs = (P("dp", None), P("comp", None), P("comp", None, None), P("comp"))
    out_specs = (P("comp", None), P("comp", None, None), P("comp"), P("dp"))
    return jax.shard_map(functools.partial(body, n_dp, n_comp), mesh=mesh, in_specs=in_specs, out_specs=out_specs, check_vma=False)
```
